8 devices in a mesh: pod: 1 (over z), data: 2 (over y), stage: 4 (over x, core).
Axes of the slice: x: 2, y: 2, z: 1, core: 2. Of those that a mesh axis runs over, the one named last changes fastest.
Arguments:
- x_last: bfloat16 [4096, 2560], P(('pod', 'data', 'stage'))
- w_head: bfloat16 [51200, 2560], P('stage')
- labels: int32 [4096], P(('pod', 'data'))
- loss_mask: int32 [4096], P(('pod', 'data'))
- w_embed: bfloat16 [51200, 2560], P('stage')
- tok_ids: int32 [4096], P(('pod', 'data'))
- act_in: bfloat16 [16384, 2560], P(('pod', 'data', 'stage'))
- w_up: bfloat16 [4, 2560, 10240], P('stage')
- w_down: bfloat16 [4, 10240, 2560], P('stage')
Outputs:
- output 1: float32 [1], P('pod')
- output 2: float32 [4096, 2560], P(('pod', 'data', 'stage'))
- output 3: bfloat16 [51200, 2560], P(('pod', 'stage'))
- output 4: bfloat16 [4096, 2560], P(('pod', 'data', 'stage'))
- output 5: bfloat16 [16384, 2560], P(('pod', 'data', 'stage'))
All inputs are finite; a program needn't handle non-finite values.
Results may differ from the reference program's by a relative error of at most 0.001.
Values are sent between devices in bfloat16 or wider.
A program may use at most 1.25 GiB of HBM per device.

```python
import jax
import jax.numpy as jnp
from jax import lax

D_MODEL = 2560
VOCAB_SIZE = 51200
D_FF = 10240
TOKENS = 2048
N_DATA = 2
N_STAGE = 4

SLICE_ROWS = VOCAB_SIZE // N_STAGE


def setup_inputs(seed: int = 0, part: int = 0) -> dict:
    base_key = jax.random.key(seed)
    shared_keys = jax.random.split(base_key, 4)
    part_keys = jax.random.split(jax.random.fold_in(base_key, part), 5)
    all_rows = N_DATA * TOKENS
    x_last = jax.random.normal(part_keys[0], (all_rows, D_MODEL), jnp.float32).astype(jnp.bfloat16)
    w_head = (2.0 * D_MODEL ** -0.5 * jax.random.normal(shared_keys[0], (VOCAB_SIZE, D_MODEL), jnp.float32)).astype(jnp.bfloat16)
    labels = jax.random.randint(part_keys[1], (all_rows,), 0, VOCAB_SIZE, jnp.int32)
    labels = labels.at[0].set(0).at[1].set(VOCAB_SIZE - 1)
    loss_mask = (jax.random.randint(part_keys[2], (all_rows,), 0, 16, jnp.int32) != 0).astype(jnp.int32)
    w_embed = jax.random.normal(shared_keys[1], (VOCAB_SIZE, D_MODEL), jnp.float32).astype(jnp.bfloat16)
    tok_ids = jax.random.randint(part_keys[3], (all_rows,), 0, VOCAB_SIZE, jnp.int32)
    tok_ids = tok_ids.at[0].set(VOCAB_SIZE - 1).at[1].set(0)
    act_in = jax.random.normal(part_keys[4], (N_DATA * N_STAGE * TOKENS, D_MODEL), jnp.float32).astype(jnp.bfloat16)
    w_up = (D_MODEL ** -0.5 * jax.random.normal(shared_keys[2], (N_STAGE, D_MODEL, D_FF), jnp.float32)).astype(jnp.bfloat16)
    w_down = (D_FF ** -0.5 * jax.random.normal(shared_keys[3], (N_STAGE, D_FF, D_MODEL), jnp.float32)).astype(jnp.bfloat16)
    return {'x_last': x_last, 'w_head': w_head, 'labels': labels, 'loss_mask': loss_mask, 'w_embed': w_embed, 'tok_ids': tok_ids, 'act_in': act_in, 'w_up': w_up, 'w_down': w_down}


def head_replica(x_rows, w_head, labels, loss_mask):
    w_slices = w_head.reshape(N_STAGE, SLICE_ROWS, D_MODEL)

    def stats_step(run_state, w_part):
        run_max, run_sum = run_state
        logits = jnp.dot(x_rows, w_part.T, preferred_element_type=jnp.float32)
        new_max = jnp.maximum(run_max, jnp.max(logits, axis=1))
        new_sum = run_sum * jnp.exp(run_max - new_max) + jnp.sum(jnp.exp(logits - new_max[:, None]), axis=1)
        return (new_max, new_sum), None

    start_state = (jnp.full((TOKENS,), -jnp.inf, jnp.float32), jnp.zeros((TOKENS,), jnp.float32))
    (row_max, row_sum), unused_out = lax.scan(stats_step, start_state, w_slices)
    weights = loss_mask.astype(jnp.float32)
    loss_denom = jnp.maximum(jnp.sum(weights), 1.0)
    target = jnp.sum(x_rows.astype(jnp.float32) * jnp.take(w_head, labels, axis=0).astype(jnp.float32), axis=1)
    rep_loss = jnp.sum(weights * (jnp.log(row_sum) + row_max - target)) / loss_denom
    row_scale = weights / loss_denom
    col_base = jnp.arange(N_STAGE, dtype=jnp.int32) * SLICE_ROWS

    def grad_step(dx_acc, step_in):
        w_part, first_col = step_in
        logits = jnp.dot(x_rows, w_part.T, preferred_element_type=jnp.float32)
        soft_probs = jnp.exp(logits - row_max[:, None]) / row_sum[:, None]
        col_ids = first_col + jnp.arange(SLICE_ROWS, dtype=jnp.int32)
        is_label = labels[:, None] == col_ids[None, :]
        grad_logits = (jnp.where(is_label, soft_probs - 1.0, soft_probs) * row_scale[:, None]).astype(jnp.bfloat16)
        dx_acc = dx_acc + jnp.dot(grad_logits, w_part, preferred_element_type=jnp.float32)
        dw_part = jnp.dot(grad_logits.T, x_rows, preferred_element_type=jnp.float32)
        return dx_acc, dw_part

    grad_rows, dw_parts = lax.scan(grad_step, jnp.zeros((TOKENS, D_MODEL), jnp.float32), (w_slices, col_base))
    return rep_loss, grad_rows, dw_parts


def reference(x_last, w_head, labels, loss_mask, w_embed, tok_ids, act_in, w_up, w_down):
    x_reps = x_last.reshape(N_DATA, TOKENS, D_MODEL)
    lab_reps = labels.reshape(N_DATA, TOKENS)
    mask_reps = loss_mask.reshape(N_DATA, TOKENS)

    def replica_step(dw_acc, rep_data):
        x_rows, rep_labels, rep_mask = rep_data
        rep_loss, grad_rows, dw_parts = head_replica(x_rows, w_head, rep_labels, rep_mask)
        return dw_acc + dw_parts, (rep_loss, grad_rows)

    dw_start = jnp.zeros((N_STAGE, SLICE_ROWS, D_MODEL), jnp.float32)
    dw_sum, (rep_losses, grad_reps) = lax.scan(replica_step, dw_start, (x_reps, lab_reps, mask_reps))
    mean_loss = (jnp.sum(rep_losses) / N_DATA).reshape(1)
    grad_x = grad_reps.reshape(N_DATA * TOKENS, D_MODEL)
    grad_head = (dw_sum / N_DATA).astype(jnp.bfloat16).reshape(VOCAB_SIZE, D_MODEL)
    embed_out = jnp.take(w_embed, tok_ids, axis=0)
    up_f32 = w_up.astype(jnp.float32)
    down_f32 = w_down.astype(jnp.float32)

    def mlp_replica(act_rep):
        act_f32 = act_rep.astype(jnp.float32)
        hidden = jax.nn.gelu(jnp.einsum('std,sdf->stf', act_f32, up_f32)).astype(jnp.bfloat16)
        out_f32 = act_f32 + jnp.einsum('stf,sfd->std', hidden.astype(jnp.float32), down_f32)
        return out_f32.astype(jnp.bfloat16)

    mlp_out = lax.map(mlp_replica, act_in.reshape(N_DATA, N_STAGE, TOKENS, D_MODEL))
    mlp_out = mlp_out.reshape(N_DATA * N_STAGE * TOKENS, D_MODEL)
    return mean_loss, grad_x, grad_head, embed_out, mlp_out
```

```python
import functools

import jax
import jax.numpy as jnp
from jax import lax
from jax.experimental import pallas as pl
from jax.experimental.pallas import tpu as pltpu
from jax.sharding import PartitionSpec as P


BF = jnp.bfloat16
F32 = jnp.float32
V = 12800
D = 2560
FF = 10240
TB = 512
PAIR = 2 * TB
ALL = 4 * TB
CB = 512
BV = 512
NT = V // BV
SUB = 8
A = 11
NR = NT - 2 * A
CALLS = ((0, (1,)), (0, (3,)), (NR, (4, 3)))
EG = 64
LANES = 2 * EG

VM = pl.BlockSpec(memory_space=pltpu.VMEM)
ANY = pl.BlockSpec(memory_space=pl.ANY)


def cdot(a, b, ca, cb):
    return lax.dot_general(a, b, (((ca,), (cb,)), ((), ())), preferred_element_type=F32)


def tree(f, xs):
    while len(xs) > 1:
        xs = [f(xs[i], xs[i + 1]) if i + 1 < len(xs) else xs[i] for i in range(0, len(xs), 2)]
    return xs[0]


def cols(k, n=TB):
    return slice(k * n, k * n + n)


def row(ref, i, c=slice(None)):
    return ref[i:i + 1, c]


def rows_at(ref, start, n):
    return ref.at[pl.ds(pl.multiple_of(start, n), n)]


def copy_all(cps):
    for c in cps:
        c.start()
    for c in cps:
        c.wait()


def params(mib=62, **kw):
    return pltpu.CompilerParams(vmem_limit_bytes=mib * 2**20, **kw)


def cost(flops, nbytes):
    return pl.CostEstimate(flops=int(flops), bytes_accessed=int(nbytes), transcendentals=0)


HEAD_COST = cost(2 * V * PAIR * D, V * D * 2 + V * PAIR * 4)


def z_body(k0, npre, *refs):
    xa_ref, xb_ref, lab_ref, w_ref = refs[:4]
    z_hbm, st_ref, m_s, s_s, t_s, zs, sem = refs[4 + npre + 1:]
    j = pl.program_id(0)
    s = lax.axis_index('stage')
    PR = PC = 128
    slot = lax.rem(j, 2)

    def out_copy(sl, jj):
        return pltpu.make_async_copy(zs.at[sl], rows_at(z_hbm, jj * BV, BV), sem.at[sl])

    @pl.when(j == 0)
    def _():
        m_s[...] = jnp.full_like(m_s, -jnp.inf)
        s_s[...] = jnp.zeros_like(s_s)
        t_s[...] = jnp.zeros_like(t_s)
        zs[...] = jnp.zeros_like(zs)

    @pl.when(j >= 2)
    def _():
        out_copy(slot, j).wait()

    io = lax.broadcasted_iota(jnp.int32, (SUB, PC), 0)

    def stats(sl, h, jj, dead=None):
        blk = pl.multiple_of((s ^ (k0 + h)) * TB, TB)
        for cc in range(TB // PC):
            c = cols(h * (TB // PC) + cc, PC)
            mo, so, to = m_s[:, c], s_s[:, c], t_s[:, c]
            lab = row(lab_ref, 0, pl.ds(blk + cc * PC, PC)) - (s * V + jj * BV)
            for rr in range(BV // PR):
                gs = [zs[sl, cols(rr * (PR // SUB) + g, SUB), c] for g in range(PR // SUB)]
                mn = jnp.maximum(mo, tree(jnp.maximum, gs))
                so = so * jnp.exp(mo - mn) + tree(jnp.add, [jnp.exp(g - mn) for g in gs])
                mo = mn
                to = to + tree(jnp.add, [jnp.where(io == lab - (rr * PR + g * SUB), v, 0.0) for g, v in enumerate(gs)])
            if dead is not None:
                mo, so, to = jnp.where(dead, -jnp.inf, mo), jnp.where(dead, 0.0, so), jnp.where(dead, 0.0, to)
            m_s[:, c], s_s[:, c], t_s[:, c] = mo, so, to

    for h, xr in enumerate((xa_ref, xb_ref)):
        stats(1 - slot, h, j - 1, j == 0)
        zs[slot, :, cols(h)] = cdot(w_ref[...], xr[...], 1, 1)
    out_copy(slot, j).start()

    @pl.when(j == NT - 1)
    def _():
        for h in range(2):
            stats(slot, h, j)
        m8 = m_s[...]
        m = jnp.max(m8, axis=0, keepdims=True)
        c = cols(npre, PAIR)
        st_ref[...] = jnp.zeros_like(st_ref)
        for i, v in enumerate((m, jnp.sum(s_s[...] * jnp.exp(m8 - m), axis=0, keepdims=True), jnp.sum(t_s[...], axis=0, keepdims=True))):
            st_ref[i:i + 1, c] = v
        if npre:
            st_ref[:, :PAIR] = refs[4][...]
        for sl in range(2):
            out_copy(sl, j).wait()


def z_call(xa, xb, lab, w, pre, dep, k0):
    pre = [] if pre is None else [pre]
    w_st = (1 + len(pre)) * PAIR
    return pl.pallas_call(
        functools.partial(z_body, k0, len(pre)),
        grid=(NT,),
        in_specs=[VM, VM, VM, pl.BlockSpec((BV, D), lambda j: (j, 0))] + [VM] * len(pre) + [ANY],
        out_specs=[ANY, VM],
        out_shape=[jax.ShapeDtypeStruct((V, PAIR), F32), jax.ShapeDtypeStruct((SUB, w_st), F32)],
        scratch_shapes=[pltpu.VMEM((SUB, PAIR), F32)] * 3 + [pltpu.VMEM((2, BV, PAIR), F32), pltpu.SemaphoreType.DMA((2,))],
        compiler_params=params(),
        cost_estimate=HEAD_COST,
    )(xa, xb, lab, w, *pre, dep)


def join_body(*refs):
    own, oth = refs[:4], refs[4:8]
    lo_ref, mo_ref, lx_ref, mx_ref, po_ref, px_ref, loss_ref = refs[8:]
    s = lax.axis_index('stage')
    total = None
    for sts, l_ref, k_ref, p_ref in ((own, lo_ref, mo_ref, po_ref), (oth, lx_ref, mx_ref, px_ref)):
        n = jnp.maximum(jnp.sum(k_ref[...].astype(F32), axis=1, keepdims=True), 1.0)
        parts = []
        for k in range(4):
            blk = pl.ds(pl.multiple_of((s ^ k) * TB, TB), TB)
            ms, ss, ts = [[row(st, i, cols(k ^ q)) for q, st in enumerate(sts)] for i in range(3)]
            m = tree(jnp.maximum, ms)
            z = tree(jnp.add, [v * jnp.exp(u - m) for u, v in zip(ms, ss)])
            t = tree(jnp.add, ts)
            mk = row(k_ref, 0, blk).astype(F32)
            sc = mk / n
            lab = (row(l_ref, 0, blk) - s * V).astype(F32)
            for i, v in enumerate((m, sc / z, sc, lab, sc, sc, sc, sc)):
                p_ref[i:i + 1, cols(k)] = v
            parts.append(jnp.sum(mk * (jnp.log(z) + m - t), axis=1, keepdims=True))
        rep = tree(jnp.add, parts) / n
        total = rep if total is None else total + rep
    loss_ref[...] = jnp.broadcast_to(total * 0.5, loss_ref.shape)


def join_call(own, oth, ints):
    return pl.pallas_call(
        join_body,
        in_specs=[VM] * 12,
        out_specs=[VM] * 3,
        out_shape=[jax.ShapeDtypeStruct((SUB, ALL), F32)] * 2 + [jax.ShapeDtypeStruct((1, 128), F32)],
        compiler_params=params(16),
        cost_estimate=cost(2e9, 2**20),
        name="join",
    )(*own, *oth, *ints)


def gfun(z, p, base):
    m, a, sc, lab = (row(p, i) for i in range(4))
    return jnp.exp(z - m) * a - jnp.where(base == lab, sc, 0.0)


def emb_body(ks, ids_ref, idv_ref, e_hbm, dep_ref, oa_ref, ob_ref, buf, cnt, sem):
    g = pl.program_id(0)
    s = lax.axis_index('stage')
    ng = TB // EG

    def issue(gg, slot):
        n = jnp.int32(0)
        for h, k in enumerate(ks):
            first = (s ^ k) * TB + gg * EG

            def one(t, c):
                i = ids_ref[first + t] - s * V
                ok = (i >= 0) & (i < V)

                @pl.when(ok)
                def _():
                    pltpu.make_async_copy(
                        rows_at(e_hbm, (i // SUB) * SUB, SUB),
                        rows_at(buf.at[slot, h], t * SUB, SUB),
                        sem.at[slot],
                    ).start()

                return c + ok.astype(jnp.int32)

            n = lax.fori_loop(0, EG, one, n, unroll=4)
        cnt[slot] = n

    @pl.when(g == 0)
    def _():
        buf[...] = jnp.zeros_like(buf)
        issue(0, 0)

    slot = lax.rem(g, 2)

    @pl.when(g + 1 < ng)
    def _():
        issue(g + 1, 1 - slot)

    def wait(t, c):
        pltpu.make_async_copy(rows_at(e_hbm, 0, SUB), rows_at(buf.at[slot, 0], 0, SUB), sem.at[slot]).wait()
        return c

    lax.fori_loop(0, cnt[slot], wait, 0)

    lane = lax.broadcasted_iota(jnp.int32, (1, LANES), 1)
    for h, (k, o) in enumerate(zip(ks, (oa_ref, ob_ref))):
        at = pl.multiple_of((s ^ k) * TB + (g // 2) * LANES, LANES)
        i = row(idv_ref, 0, pl.ds(at, LANES)) - s * V
        i = jnp.where((i >= 0) & (i < V), (lane % EG) * SUB + i % SUB, -1)
        i = jnp.where(slot == 0, i[:, :EG], i[:, EG:])
        oh = (lax.broadcasted_iota(jnp.int32, (EG * SUB, EG), 0) == i).astype(F32).astype(BF)
        o[...] = cdot(oh, buf[slot, h], 0, 0).astype(BF)


def emb_call(ids, e, dep, ks):
    gs = pltpu.PrefetchScalarGridSpec(
        num_scalar_prefetch=1,
        grid=(TB // EG,),
        in_specs=[VM, ANY, ANY],
        out_specs=[pl.BlockSpec((EG, D), lambda g, *_: (g, 0))] * 2,
        scratch_shapes=[pltpu.VMEM((2, 2, EG * SUB, D), BF), pltpu.SMEM((2,), jnp.int32), pltpu.SemaphoreType.DMA((2,))],
    )
    return pl.pallas_call(
        functools.partial(emb_body, ks),
        grid_spec=gs,
        out_shape=[jax.ShapeDtypeStruct((TB, D), BF)] * 2,
        compiler_params=params(),
        cost_estimate=cost(1e10, 2**24),
    )(ids, ids.reshape(1, -1), e, dep)


def d_body(nr, c0, sizes, off_ref, *refs):
    ns = len(sizes)
    xs_hbm, (po_ref, px_ref, z1_ref, z2_ref, w_ref) = refs[:8], refs[8:13]
    xs, gt, ob, xsem, osem = refs[-5:]
    g_hbm, *snd = refs[-6 - ns:-5]
    j = pl.program_id(0)
    nt = nr + sum(sizes)
    r = off_ref[1]
    own = pl.multiple_of(r * ALL, ALL)
    oth = pl.multiple_of((1 - r) * ALL, ALL)
    tile = jnp.where(j < nr, 2 * A + j, off_ref[0] + c0 + j - nr)
    slot = lax.rem(j, 2)

    def out_copy(dst, at, sl, which):
        return pltpu.make_async_copy(ob.at[sl], rows_at(dst, at, BV), osem.at[sl, which])

    @pl.when(j == 0)
    def _():
        copy_all([pltpu.make_async_copy(x, rows_at(xs, (own if i < 4 else oth) + (i % 4) * TB, TB), xsem.at[i])
                  for i, x in enumerate(xs_hbm)])

    @pl.when(j >= 2)
    def _():
        out_copy(g_hbm, 0, slot, 0).wait()

    @pl.when(j >= 2 + nr)
    def _():
        out_copy(snd[0], 0, slot, 1).wait()

    base = (lax.broadcasted_iota(jnp.int32, (BV, 1), 0) + tile * BV).astype(F32)
    for tb in range(4):
        zr = (z1_ref, z2_ref)[tb // 2]
        gt[:, pl.ds(own + tb * TB, TB)] = gfun(zr[:, cols(tb % 2)], po_ref[:, cols(tb)], base).astype(BF)
    for tb in range(4):
        zt = cdot(w_ref[...], xs[pl.ds(oth + tb * TB, TB), :], 1, 1)
        gt[:, pl.ds(oth + tb * TB, TB)] = gfun(zt, px_ref[:, cols(tb)], base).astype(BF)
    for n in range(D // CB):
        ob[slot, :, cols(n, CB)] = (cdot(gt[...], xs[:, cols(n, CB)], 1, 0) * 0.5).astype(BF)

    out_copy(g_hbm, tile * BV, slot, 0).start()
    lo = nr
    for i, sz in enumerate(sizes):
        @pl.when((j >= lo) & (j < lo + sz))
        def _(i=i, lo=lo):
            out_copy(snd[i], (j - lo) * BV, slot, 1).start()

        lo += sz

    @pl.when(j == nt - 1)
    def _():
        for jj in range(max(nt - 2, 0), nt):
            for which, dst in enumerate((g_hbm, snd[0])[:1 + (jj >= nr)]):
                out_copy(dst, 0, jj % 2, which).wait()


def d_call(off, xs, po, px, z1, z2, w, gin, dep, nr, c0, sizes):
    nt = nr + sum(sizes)
    tile = lambda j, o: (jnp.where(j < nr, 2 * A + j, o[0] + c0 + j - nr), 0)
    ins = [off, *xs, po, px, z1, z2, w]
    specs = [ANY] * 8 + [VM, VM] + [pl.BlockSpec((BV, PAIR), tile)] * 2 + [pl.BlockSpec((BV, D), tile)]
    alias = {}
    if gin is not None:
        alias = {len(ins): 0}
        ins.append(gin)
        specs.append(ANY)
    ins.append(dep)
    specs.append(ANY)
    gs = pltpu.PrefetchScalarGridSpec(
        num_scalar_prefetch=1,
        grid=(nt,),
        in_specs=specs,
        out_specs=[ANY] * (1 + len(sizes)),
        scratch_shapes=[
            pltpu.VMEM((2 * ALL, D), BF),
            pltpu.VMEM((BV, 2 * ALL), BF),
            pltpu.VMEM((2, BV, D), BF),
            pltpu.SemaphoreType.DMA((8,)),
            pltpu.SemaphoreType.DMA((2, 2)),
        ],
    )
    return pl.pallas_call(
        functools.partial(d_body, nr, c0, sizes),
        grid_spec=gs,
        out_shape=[jax.ShapeDtypeStruct((V, D), BF)] + [jax.ShapeDtypeStruct((s * BV, D), BF) for s in sizes],
        input_output_aliases=alias,
        compiler_params=params(),
        cost_estimate=cost(nt * 6 * BV * ALL * D, nt * 12e6 + 21e6),
    )(*ins)


def dx_body(half, p_ref, za0, zb0, zan, zbn, w0, wn, w1, w2, w3, w4, dep_ref, oa_ref, ob_ref, acc, g0, g1, sem):
    j = pl.program_id(0)

    def mkg(dst, za, zb, tile):
        base = (lax.broadcasted_iota(jnp.int32, (BV, 1), 0) + tile * BV).astype(F32)
        for k in range(BV // LANES):
            c = cols(k, LANES)
            for q, zr in enumerate((za, zb)):
                dst[cols(q), c] = gfun(zr[c, :], p_ref[:, cols(half + 2 * q)], base[c]).astype(BF).T

    @pl.when(j == 0)
    def _():
        mkg(g0, za0, zb0, 0)
        acc[...] = jnp.zeros_like(acc)
        acc[:, :CB] = cdot(g0[...], w0[...], 1, 0)

    def step(cur, nxt):
        mkg(nxt, zan, zbn, j + 1)
        for i, w in enumerate((w1, w2, w3, w4)):
            acc[:, cols(i + 1, CB)] += cdot(cur[...], w[...], 1, 0)
        acc[:, :CB] += jnp.where(j == NT - 1, 0.0, cdot(nxt[...], wn[...], 1, 0))

    @pl.when(lax.rem(j, 2) == 0)
    def _():
        step(g0, g1)

    @pl.when(lax.rem(j, 2) == 1)
    def _():
        step(g1, g0)

    @pl.when(j == NT - 1)
    def _():
        copy_all([pltpu.make_async_copy(acc.at[cols(i)], o, sem.at[i]) for i, o in enumerate((oa_ref, ob_ref))])


def dx_call(p, z1, z2, w, dep, half):
    zs = lambda im, **k: pl.BlockSpec((BV, TB), im, **k)
    first = zs(lambda j: (0, half), pipeline_mode=pl.Buffered(1))
    nj = lambda j: jnp.minimum(j + 1, NT - 1)
    nxt = zs(lambda j: (nj(j), half))
    ws = [pl.BlockSpec((BV, CB), lambda j: (0, 0), pipeline_mode=pl.Buffered(1)), pl.BlockSpec((BV, CB), lambda j: (nj(j), 0))]
    ws += [pl.BlockSpec((BV, CB), lambda j, q=q: (j, q)) for q in range(1, D // CB)]
    return pl.pallas_call(
        functools.partial(dx_body, half),
        grid=(NT,),
        in_specs=[VM, first, first, nxt, nxt] + ws + [ANY],
        out_specs=[ANY, ANY],
        out_shape=[jax.ShapeDtypeStruct((TB, D), F32)] * 2,
        scratch_shapes=[pltpu.VMEM((PAIR, D), F32)] + [pltpu.VMEM((PAIR, BV), BF)] * 2 + [
            pltpu.SemaphoreType.DMA((2,))],
        compiler_params=params(),
        cost_estimate=HEAD_COST,
    )(p, z1, z2, z1, z2, *([w] * 6), dep)


def mlp_body(nsrc, split, fb, mb, off_ref, a_ref, w1_ref, w2_ref, *refs):
    src = refs[:nsrc]
    o_ref, g_ref, acc, h_s = refs[nsrc + 2:]
    j = pl.program_id(0)
    rows = PAIR
    n = FF // fb
    nb = rows // mb
    g_ref[...] = src[0][...] if nsrc == 1 else jnp.where(j < split, src[0][...], src[1][...])

    def d1(b):
        r = cols(b, mb)
        h_s[r, :] = jax.nn.gelu(cdot(a_ref[r, :], w1_ref[0], 1, 0)).astype(BF)

    def d2(b):
        r = cols(b, mb)
        for i in range(D // CB):
            c = cols(i, CB)
            acc[r, c] = jnp.where(j == 0, a_ref[r, c].astype(F32), acc[r, c]) + cdot(h_s[r, :], w2_ref[0, :, c], 1, 0)

    d1(0)
    for b in range(1, nb):
        d1(b)
        d2(b - 1)
    d2(nb - 1)

    @pl.when(j == n - 1)
    def _():
        o_ref[...] = acc[...].astype(BF)


def mlp_call(off, a, w1, w2, srcs, gin, dep, row_blk, c0, oin=None, fb=512, mb=256, cb=128):
    n = FF // fb
    rows = PAIR
    nblk = [s.shape[0] // cb for s in srcs]
    tot = sum(nblk)
    split = nblk[0]
    sspecs = [pl.BlockSpec((cb, D), lambda j, o: (jnp.minimum(j, nblk[0] - 1), 0))]
    if len(srcs) > 1:
        sspecs.append(pl.BlockSpec((cb, D), lambda j, o: (jnp.clip(j - split, 0, nblk[1] - 1), 0)))
    t = BV // cb
    gs = pltpu.PrefetchScalarGridSpec(
        num_scalar_prefetch=1,
        grid=(n,),
        in_specs=[pl.BlockSpec((rows, D), lambda j, o: (row_blk, 0), pipeline_mode=pl.Buffered(1)),
                  pl.BlockSpec((1, D, fb), lambda j, o: (0, 0, j)),
                  pl.BlockSpec((1, fb, D), lambda j, o: (0, j, 0))] + sspecs + [ANY, ANY],
        out_specs=[pl.BlockSpec((rows, D), lambda j, o: (row_blk, 0), pipeline_mode=pl.Buffered(1)),
                   pl.BlockSpec((cb, D), lambda j, o: ((A - o[0] + c0) * t + jnp.minimum(j, tot - 1), 0))],
        scratch_shapes=[pltpu.VMEM((rows, D), F32), pltpu.VMEM((rows, fb), BF)],
    )
    k = 4 + len(srcs)
    alias = {k: 1}
    if oin is not None:
        alias[k + 1] = 0
        dep = oin
    return pl.pallas_call(
        functools.partial(mlp_body, len(srcs), split, fb, mb),
        grid_spec=gs,
        out_shape=[jax.ShapeDtypeStruct((ALL, D), BF), jax.ShapeDtypeStruct((V, D), BF)],
        input_output_aliases=alias,
        compiler_params=params(),
        cost_estimate=cost(4 * rows * FF * D, 110e6),
    )(off, a, w1, w2, *srcs, gin, dep)


def put_body(off_ref, s_ref, gin_ref, g_ref):
    g_ref[...] = s_ref[...]


def put_call(off, src, gin, c0, cb=256):
    n = src.shape[0] // cb
    gs = pltpu.PrefetchScalarGridSpec(
        num_scalar_prefetch=1,
        grid=(n,),
        in_specs=[pl.BlockSpec((cb, D), lambda j, o: (j, 0)), ANY],
        out_specs=pl.BlockSpec((cb, D), lambda j, o: ((A - o[0] + c0) * (BV // cb) + j, 0)),
    )
    return pl.pallas_call(
        put_body,
        grid_spec=gs,
        out_shape=jax.ShapeDtypeStruct((V, D), BF),
        input_output_aliases={2: 0},
        compiler_params=params(),
        cost_estimate=cost(1e9, 2 * src.size * 2),
        name="put",
    )(off, src, gin)


def solution(mesh):
    tok_spec = P(('pod', 'data', 'stage'), None)
    rep_spec = P(('pod', 'data'))
    vocab_spec = P('stage', None)
    layer_spec = P('stage', None, None)

    def px(a, q):
        return lax.ppermute(a, 'stage', [(i, i ^ q) for i in range(4)])

    def py(a, q=0):
        if q == 0:
            return lax.ppermute(a, 'data', [(0, 1), (1, 0)])
        return lax.ppermute(a, ('data', 'stage'), [(i, i ^ 4 ^ q) for i in range(8)])

    def local_step(x, w_head, labels, loss_mask, w_embed, tok_ids, act_in, w_up, w_down):
        r = lax.axis_index('data')
        off = jnp.stack([r * A, r]).astype(jnp.int32)

        x1 = px(x, 1)
        x2 = px(x, 2)
        xo0 = py(x)
        x3 = px(x2, 1)
        xo2 = px(xo0, 2)
        xo1 = px(xo0, 1)
        xo3 = px(xo2, 1)
        lab = labels.reshape(1, -1)
        msk = loss_mask.reshape(1, -1)
        labx = py(lab)
        mskx = py(msk)

        z1, st1 = z_call(x, x1, lab, w_head, None, x, 0)
        e1, e3 = emb_call(tok_ids, w_embed, st1, (1, 3))
        z2, st = z_call(x2, x3, lab, w_head, st1, e1, 2)
        own = [px(st, q) if q else st for q in range(4)]
        oth = [py(st, q) for q in range(4)]
        re1 = px(e1, 1)
        re3 = px(e3, 1)
        e0, e2 = emb_call(tok_ids, w_embed, st, (0, 2))
        po, pxx, loss = join_call(own, oth, [lab, msk, labx, mskx])
        re2 = px(e2 + re3, 2)

        xs = [x, x1, x2, x3, xo0, xo1, xo2, xo3]
        g, rcv, at = None, [], []
        for i, (nr, sizes) in enumerate(CALLS):
            c0 = sum(sum(q) for _, q in CALLS[:i])
            g, *snd = d_call(off, xs, po, pxx, z1, z2, w_head, g, e0, nr, c0, sizes)
            for a, q in zip(snd, sizes):
                rcv.append(py(a))
                at.append(c0)
                c0 += q

        dx1, dx3 = dx_call(po, z1, z2, w_head, g, 1)
        rd1 = px(dx1, 1)
        rd3 = px(dx3, 1)
        dx0, dx2 = dx_call(po, z1, z2, w_head, dx1, 0)
        rd2 = px(dx2 + rd3, 2)

        m, g = mlp_call(off, act_in, w_up, w_down, rcv[:2], g, dx0, 0, at[0])
        m, g = mlp_call(off, act_in, w_up, w_down, rcv[2:3], g, m, 1, at[2], oin=m)
        g = put_call(off, rcv[3], g, at[3])

        grad_x = (dx0 + rd1) + rd2
        emb = (e0 + re1) + re2
        return loss[0, :1], grad_x, g, emb, m

    return jax.shard_map(
        local_step,
        mesh=mesh,
        in_specs=(tok_spec, vocab_spec, rep_spec, rep_spec, vocab_spec, rep_spec, tok_spec, layer_spec, layer_spec),
        out_specs=(P('pod'), tok_spec, P(('pod', 'stage'), None), tok_spec, tok_spec),
        check_vma=False,
    )
```
